32 devices in a mesh: gx: 4 (over y, core), gy: 2 (over x), gz: 4 (over z).
Axes of the slice: x: 2, y: 2, z: 4, core: 2. Of those that a mesh axis runs over, the one named last changes fastest.
Arguments:
- pressure_now: float32 [64, 64, 512], P('gx', 'gy', 'gz'), may hold values from -6 to 6
- pressure_before: float32 [64, 64, 512], P('gx', 'gy', 'gz'), may hold values from -6 to 6
- region_code: int32 [64, 64, 512], P('gx', 'gy', 'gz'), may hold values from 0 to 7
- velocity: float32 [8], replicated, may hold values from 0.2 to 0.42
- wavelet: float32 [6, 16], replicated, may hold values from -6 to 6
- source_cell: int32 [16], replicated, may hold values from 0 to 2097151
Outputs:
- pressure: float32 [64, 64, 512], P('gx', 'gy', 'gz')
- previous: float32 [64, 64, 512], P('gx', 'gy', 'gz')
The draws below stay inside these ranges and needn't reach their ends.
Inputs may be any that keep to these rules, and one draw needn't show every extreme that they name: source_cell[s] is the flat index x * 64 * 512 + y * 512 + z of a grid cell; sources may share a cell.
All inputs are finite; a program needn't handle non-finite values.
Results may differ from the reference program's by a relative error of at most 0.00002.
Values sent between devices are 32-bit elements; how exact they have to be, the bound alone decides.
A program may use at most 64 MiB of HBM per device.

```python
import math
import jax
import jax.numpy as jnp
from jax import lax

STEPS = 6
NSRC = 16
NREG = 8
NX = 64
NY = 64
NZ = 512


def touch_ends(array, rng, least, top_value):
    extent = array.shape
    place = [jax.random.randint(jax.random.fold_in(rng, axis), (), 0, extent[axis]) for axis in range(len(extent))]
    array = array.at[tuple(place)].set(least)
    longest = extent.index(max(extent))
    place[longest] = (place[longest] + 1) % extent[longest]
    return array.at[tuple(place)].set(top_value)


def steps_of(rng, dims, cuts, low, largest):
    factor_of, own = 1.0, jax.random.fold_in(rng, 6)
    for position, blocks in cuts:
        steps = jnp.exp(jax.random.uniform(jax.random.fold_in(own, position), (blocks,), jnp.float32, low / len(cuts), largest / len(cuts)))
        factor_of = factor_of * jnp.repeat(steps, dims[position] // blocks).reshape([-1 if axis == position else 1 for axis in range(len(dims))])
    return factor_of


def noise(own_key, extent, spread, limit, split=(), dtype=jnp.bfloat16):
    level = steps_of(own_key, extent, split, -0.22, 0.18) if split else 1.0
    result = jax.random.normal(own_key, extent, jnp.float32) * spread * level
    return jnp.minimum(jnp.maximum(result, -limit), limit).astype(dtype)


def setup_inputs(seed: int = 0) -> dict:
    splits = jax.random.split(jax.random.key(seed), 7)
    return {
        "pressure_now": noise(splits[0], (NX, NY, NZ), 1.0, 6.0, ((0, 4), (1, 2), (2, 4)), jnp.float32),
        "pressure_before": noise(splits[1], (NX, NY, NZ), 1.0, 6.0, ((0, 4), (1, 2), (2, 4)), jnp.float32),
        "region_code": touch_ends(jax.random.randint(splits[2], (NX, NY, NZ), 0, NREG), jax.random.fold_in(splits[2], 1), 0, NREG - 1).astype(jnp.int32),
        "velocity": jnp.clip(jnp.exp(jax.random.uniform(splits[3], (NREG,), jnp.float32, math.log(0.2), math.log(0.42))), 0.2, 0.42),
        "wavelet": noise(splits[4], (STEPS, NSRC), 1.0, 6.0, (), jnp.float32),
        "source_cell": touch_ends(jax.random.randint(splits[5], (NSRC,), 0, NX * NY * NZ), jax.random.fold_in(splits[5], 1), 0, (NX * NY * NZ) - 1).astype(jnp.int32),
    }


CENTRE = -205.0 / 72.0
WEIGHTS = (8.0 / 5.0, -1.0 / 5.0, 8.0 / 315.0, -1.0 / 560.0)


def cut(field, start, size):
    return lax.slice(field, tuple(start), tuple(a + b for a, b in zip(start, size)))


def along(field, axis, start, size):
    total = None
    for step_k, weight in enumerate(WEIGHTS, 1):
        upper = list(start)
        upper[axis] = upper[axis] + step_k
        lower = list(start)
        lower[axis] = lower[axis] - step_k
        term = weight * (cut(field, upper, size) + cut(field, lower, size))
        total = term if total is None else total + term
    return total


def reference(pressure_now, pressure_before, region_code, velocity, wavelet, source_cell):
    size = pressure_now.shape
    speed = velocity[region_code]
    rate = speed * speed
    current = pressure_now
    before = pressure_before
    for step in range(STEPS):
        padded = jnp.pad(current, ((4, 4), (0, 0), (0, 0)), mode="wrap")
        padded = jnp.pad(padded, ((0, 0), (4, 4), (4, 4)))
        start = (4, 4, 4)
        laplace = 3.0 * CENTRE * current + along(padded, 0, start, size) + along(padded, 1, start, size) + along(padded, 2, start, size)
        following = 2.0 * current - before + rate * laplace
        following = following.reshape(-1).at[source_cell].add(wavelet[step]).reshape(size)
        before = current
        current = following
    return current, before
```

```python
import functools

import jax
import jax.numpy as jnp
from jax import lax
from jax.experimental import pallas as pl
from jax.experimental.pallas import tpu as pltpu
from jax.sharding import PartitionSpec as P

STEPS = 6
CENTRE = -205.0 / 72.0
C1, C2, C3, C4 = (8.0 / 5.0, -1.0 / 5.0, 8.0 / 315.0, -1.0 / 560.0)
WEIGHTS = (C1, C2, C3, C4)
W = 4
T = 8
LANES = 128
MESH = pl.DeviceIdType.MESH


def kernel(sizes, now_hbm, before_hbm, code_hbm, vel_ref, wave_ref, src_ref,
           out_hbm, prev_hbm, field, rate, code, source, pack, edge, send_sem, recv_sem, load_sem, store_sem):
    (nx, ny, nz), (gx, gy, gz) = sizes
    grid_y, grid_z = ny * gy, nz * gz
    ix, iy, iz = lax.axis_index("gx"), lax.axis_index("gy"), lax.axis_index("gz")
    x_low, x_high = lax.rem(ix + gx - 1, gx), lax.rem(ix + 1, gx)
    targets = (
        ({"gx": x_low}, None),
        ({"gx": x_high}, None),
        ({"gy": iy - 1}, iy > 0),
        ({"gy": iy + 1}, iy < gy - 1),
        ({"gz": iz - 1}, iz > 0),
        ({"gz": iz + 1}, iz < gz - 1),
    )

    def guarded(condition, action):
        if condition is None:
            action()
        else:
            pl.when(condition)(action)

    own_x, own_y = pl.ds(W, nx), pl.ds(T, ny)
    loads = [
        pltpu.make_async_copy(now_hbm, field.at[0, own_x, own_y], load_sem.at[0]),
        pltpu.make_async_copy(before_hbm, field.at[1, own_x, own_y], load_sem.at[1]),
        pltpu.make_async_copy(code_hbm, code, load_sem.at[2]),
    ]
    for load in loads:
        load.start()

    nothing = jnp.zeros((nx, T, LANES), jnp.float32)
    for par in range(2):
        field[par, own_x, 0:T, :] = nothing
        field[par, own_x, pl.ds(T + ny, T), :] = nothing
    edge[...] = jnp.zeros_like(edge)

    barrier = pltpu.get_barrier_semaphore()
    for target, present in targets:
        guarded(present, lambda target=target: pl.semaphore_signal(
            barrier, inc=1, device_id=target, device_id_type=MESH))

    def copies(par):
        pairs = (
            (field.at[par, pl.ds(W, W), own_y], field.at[par, pl.ds(W + nx, W), own_y]),
            (field.at[par, pl.ds(nx, W), own_y], field.at[par, pl.ds(0, W), own_y]),
            (field.at[par, own_x, pl.ds(T, T)], field.at[par, own_x, pl.ds(T + ny, T)]),
            (field.at[par, own_x, pl.ds(ny, T)], field.at[par, own_x, pl.ds(0, T)]),
            (pack.at[par], edge.at[par, 1]),
            (pack.at[par], edge.at[par, 0]),
        )
        return [
            pltpu.make_async_remote_copy(
                src_ref=src, dst_ref=dst, send_sem=send_sem.at[par, n], recv_sem=recv_sem.at[par, n],
                device_id=target, device_id_type=MESH)
            for n, ((src, dst), (target, _)) in enumerate(zip(pairs, targets))
        ]

    def start(par):
        for copy, (_, present) in zip(copies(par), targets):
            guarded(present, copy.start)

    def wait_send(par):
        for copy, (_, present) in zip(copies(par), targets):
            guarded(present, copy.wait_send)

    def wait_recv(par):
        opposite = (1, 0, 3, 2, 5, 4)
        for n, copy in enumerate(copies(par)):
            guarded(targets[opposite[n]][1], copy.wait_recv)

    lane = lax.broadcasted_iota(jnp.int32, (8, LANES), 1)
    group_of, place = lane // 8, lane % 8
    per_pack = LANES // 8
    slabs = per_pack // 4
    packs = nx // slabs

    def packed(value, g, total):
        return jnp.where(group_of == g, pltpu.roll(value, (W + 8 * g) % LANES, 1), total)

    def rows(j):
        return pl.ds(T + j, 8, stride=4)

    loads[0].wait()

    def first_pack(m, carry):
        total = jnp.zeros((8, LANES), jnp.float32)
        for a in range(slabs):
            for j in range(4):
                total = packed(field[0, W + m * slabs + a, rows(j), :], a * 4 + j, total)
        pack[0, m] = total
        return carry

    lax.fori_loop(0, packs, first_pack, 0)
    peers = 2
    for _, present in targets[2:]:
        peers = peers + present.astype(jnp.int32)
    pl.semaphore_wait(barrier, peers)
    start(0)

    loads[2].wait()
    squares = [vel_ref[n] * vel_ref[n] for n in range(vel_ref.shape[0])]

    def rate_slab(x, carry):
        codes = code[x]
        value = jnp.full(codes.shape, squares[0], jnp.float32)
        for n in range(1, len(squares)):
            value = jnp.where(codes == n, squares[n], value)
        rate[x] = value
        return carry

    lax.fori_loop(0, nx, rate_slab, 0)

    count = src_ref.shape[0]
    row_at = jnp.full((1, LANES), -1, jnp.int32)
    lane_row = lax.broadcasted_iota(jnp.int32, (1, LANES), 1)
    slot_col = lax.broadcasted_iota(jnp.int32, (LANES, LANES), 0)
    z_at = jnp.full((LANES, LANES), -1, jnp.int32)
    for s in range(count):
        cell = src_ref[s]
        sx = cell // (grid_y * grid_z) - ix * nx
        sy = cell // grid_z % grid_y - iy * ny
        sz = cell % grid_z - iz * nz
        here = (sx >= 0) & (sx < nx) & (sy >= 0) & (sy < ny)
        local = jnp.where(here, sx * ny + sy, -1)
        row_at = jnp.where((lane_row % count == s) & (lane_row < 3 * count), local, row_at)
        z_at = jnp.where((slot_col % count == s) & (slot_col < 3 * count), sz, z_at)
    spread = (z_at == lax.broadcasted_iota(jnp.int32, (LANES, LANES), 1)).astype(jnp.float32).astype(jnp.bfloat16)

    def source_field(t):
        wave = jnp.zeros((1, LANES), jnp.float32)
        for s in range(count):
            wave = jnp.where(lane_row % count == s, wave_ref[t, s], wave)
        high = wave.astype(jnp.bfloat16).astype(jnp.float32)
        rest = wave - high
        middle = rest.astype(jnp.bfloat16).astype(jnp.float32)
        parts = jnp.where(lane_row < count, high, jnp.where(lane_row < 2 * count, middle, rest - middle))
        block = slabs * ny

        def chunk(m, carry):
            row = lax.broadcasted_iota(jnp.int32, (block, LANES), 0) + m * block
            picks = jnp.where(row == row_at, parts, 0.0).astype(jnp.bfloat16)
            value = jnp.dot(picks, spread, preferred_element_type=jnp.float32)
            source[pl.ds(m * slabs, slabs)] = value.reshape(slabs, ny, LANES)
            return carry

        lax.fori_loop(0, packs, chunk, 0)

    near_edge = (lane < W) | (lane >= LANES - W)
    take_up = [jnp.where((place >= W) & (place - k < W), WEIGHTS[k - 1], 0.0) for k in range(1, W + 1)]
    take_down = [jnp.where((place < W) & (place + k >= W), WEIGHTS[k - 1], 0.0) for k in range(1, W + 1)]

    loads[1].wait()
    for t in range(STEPS):
        cur, nxt = t % 2, (t + 1) % 2
        source_field(t)
        if t >= 1:
            wait_send(nxt)
        wait_recv(cur)

        def block(m, carry):
            delta = jnp.where(place < W, edge[cur, 0, m], edge[cur, 1, m]) - pack[cur, m]
            fix = jnp.zeros((8, LANES), jnp.float32)
            for k in range(1, W + 1):
                fix = fix + take_up[k - 1] * pltpu.roll(delta, k, 1)
                fix = fix + take_down[k - 1] * pltpu.roll(delta, LANES - k, 1)
            total = jnp.zeros((8, LANES), jnp.float32)
            for a in range(slabs):
                x = m * slabs + a
                shifted = [field[cur, W + x, pl.ds(W + o, 8, stride=4), :] for o in range(12)]
                for j in range(4):
                    g = a * 4 + j
                    f = shifted[4 + j]
                    acc = (3.0 * CENTRE) * f
                    for k in range(1, W + 1):
                        acc = acc + WEIGHTS[k - 1] * (
                            (field[cur, W + x + k, rows(j), :] + field[cur, W + x - k, rows(j), :])
                            + (shifted[4 + j + k] + shifted[4 + j - k]))
                    below, above = pltpu.roll(f, 1, 1), pltpu.roll(f, LANES - 1, 1)
                    far_below = C4 * below + C3 * f + C2 * above
                    far_above = C2 * below + C3 * f + C4 * above
                    acc = acc + C1 * (below + above)
                    acc = acc + pltpu.roll(far_below, 3, 1) + pltpu.roll(far_above, LANES - 3, 1)
                    acc = acc + jnp.where(near_edge, pltpu.roll(fix, (2 * LANES - W - 8 * g) % LANES, 1), 0.0)
                    own = pl.ds(j, 8, stride=4)
                    value = (2.0 * f - field[nxt, W + x, rows(j), :]) + rate[x, own, :] * acc + source[x, own, :]
                    field[nxt, W + x, rows(j), :] = value
                    if t < STEPS - 1:
                        total = packed(value, g, total)
            if t < STEPS - 1:
                pack[nxt, m] = total
            return carry

        lax.fori_loop(0, packs, block, 0)
        if t < STEPS - 1:
            start(nxt)
        if t == STEPS - 2:
            store_prev = pltpu.make_async_copy(field.at[nxt, own_x, own_y], prev_hbm, store_sem.at[0])
            store_prev.start()
    store_out = pltpu.make_async_copy(field.at[STEPS % 2, own_x, own_y], out_hbm, store_sem.at[1])
    store_out.start()
    wait_send((STEPS - 1) % 2)
    store_prev.wait()
    store_out.wait()


def solution(mesh):
    counts = tuple(mesh.shape[name] for name in ("gx", "gy", "gz"))

    def per_device(now, before, codes, velocity, wavelet, source_cell):
        nx, ny, nz = now.shape
        anywhere = pl.BlockSpec(memory_space=pl.ANY)
        scalars = pl.BlockSpec(memory_space=pltpu.SMEM)
        packs = nx * ny // LANES
        return pl.pallas_call(
            functools.partial(kernel, (now.shape, counts)),
            out_shape=(jax.ShapeDtypeStruct(now.shape, jnp.float32),) * 2,
            in_specs=[anywhere] * 3 + [scalars] * 3,
            out_specs=(anywhere, anywhere),
            scratch_shapes=[
                pltpu.VMEM((2, nx + 2 * W, ny + 2 * T, nz), jnp.float32),
                pltpu.VMEM((nx, ny, nz), jnp.float32),
                pltpu.VMEM((nx, ny, nz), jnp.int32),
                pltpu.VMEM((nx, ny, nz), jnp.float32),
                pltpu.VMEM((2, packs, 8, LANES), jnp.float32),
                pltpu.VMEM((2, 2, packs, 8, LANES), jnp.float32),
                pltpu.SemaphoreType.DMA((2, 6)),
                pltpu.SemaphoreType.DMA((2, 6)),
                pltpu.SemaphoreType.DMA((3,)),
                pltpu.SemaphoreType.DMA((2,)),
            ],
            compiler_params=pltpu.CompilerParams(collective_id=0, has_side_effects=True),
        )(now, before, codes, velocity, wavelet, source_cell)

    block = P("gx", "gy", "gz")
    return jax.shard_map(
        per_device,
        mesh=mesh,
        in_specs=(block, block, block, P(), P(), P()),
        out_specs=(block, block),
        check_vma=False,
    )
```

```python
import functools

import jax
import jax.numpy as jnp
from jax import lax
from jax.experimental import pallas as pl
from jax.experimental.pallas import tpu as pltpu
from jax.sharding import PartitionSpec as P

STEPS = 6
CENTRE = -205.0 / 72.0
C1, C2, C3, C4 = (8.0 / 5.0, -1.0 / 5.0, 8.0 / 315.0, -1.0 / 560.0)
WEIGHTS = (C1, C2, C3, C4)
W = 4
T = 8
LANES = 128
MESH = pl.DeviceIdType.MESH
def kernel(sizes, now_hbm, before_hbm, code_hbm, vel_ref, wave_ref, src_ref, out_ref, prev_ref,
           field, face, halo, rate, code, source, pack, edge, send_sem, recv_sem, load_sem):
    (nx, ny, nz), (gx, gy, gz) = sizes
    grid_y, grid_z = ny * gy, nz * gz
    lanes_of = ny // 8
    slabs = LANES // 8 // lanes_of
    packs = nx // slabs
    ix, iy, iz = lax.axis_index("gx"), lax.axis_index("gy"), lax.axis_index("gz")
    targets = (
        (({"gx": lax.rem(ix + gx - 1, gx)}, None), ({"gx": lax.rem(ix + 1, gx)}, None)),
        (({"gy": iy - 1}, iy > 0), ({"gy": iy + 1}, iy < gy - 1)),
        (({"gz": iz - 1}, iz > 0), ({"gz": iz + 1}, iz < gz - 1)),
    )

    def guarded(condition, action):
        if condition is None:
            action()
        else:
            pl.when(condition)(action)

    own_x, own_y = pl.ds(0, nx), pl.ds(T, ny)
    loads = [
        pltpu.make_async_copy(now_hbm, field.at[0, own_x, own_y], load_sem.at[0]),
        pltpu.make_async_copy(before_hbm, field.at[1, own_x, own_y], load_sem.at[1]),
        pltpu.make_async_copy(code_hbm, code, load_sem.at[2]),
    ]
    for load in loads:
        load.start()

    nothing = jnp.zeros((nx, T, LANES), jnp.float32)
    for par in range(2):
        field[par, own_x, 0:T, :] = nothing
        field[par, own_x, pl.ds(T + ny, T), :] = nothing
    edge[...] = jnp.zeros_like(edge)

    barrier = pltpu.get_barrier_semaphore()
    for sides in targets:
        for target, present in sides:
            guarded(present, lambda target=target: pl.semaphore_signal(
                barrier, inc=1, device_id=target, device_id_type=MESH))

    inner = packs - 2

    def group(name, par):
        pieces = []
        if name[0] == "x":
            n = name[1]
            base = 2 * n
            pieces = [(0, face.at[par, 0, n], halo.at[par, 1, n]), (0, face.at[par, 1, n], halo.at[par, 0, n])]
        else:
            axis = 1 if name[0] == "y" else 2
            base = 2 * lanes_of + (0 if axis == 1 else 6)
            if axis == 1:
                low, high = pl.ds(T, T), pl.ds(ny, T)
                over, under = pl.ds(T + ny, T), pl.ds(0, T)
                if name[1] == "face":
                    spans = [pl.ds(0, slabs), pl.ds(nx - slabs, slabs)]
                else:
                    spans = [pl.ds(slabs, nx - 2 * slabs)]
                    base = base + 4
                for span in spans:
                    pieces.append((1, field.at[par, span, low], field.at[par, span, over]))
                    pieces.append((1, field.at[par, span, high], field.at[par, span, under]))
            else:
                span = pl.ds(0, 2) if name[1] == "face" else pl.ds(2, inner)
                base = base + (0 if name[1] == "face" else 2)
                pieces.append((2, pack.at[par, span], edge.at[par, 1, span]))
                pieces.append((2, pack.at[par, span], edge.at[par, 0, span]))
        result = []
        for n, (axis, src, dst) in enumerate(pieces):
            target, present = targets[axis][n % 2]
            copy = pltpu.make_async_remote_copy(
                src_ref=src, dst_ref=dst, send_sem=send_sem.at[par, base + n], recv_sem=recv_sem.at[par, base + n],
                device_id=target, device_id_type=MESH)
            result.append((copy, present, targets[axis][1 - n % 2][1]))
        return result

    def start(name, par):
        for copy, to_here, _ in group(name, par):
            guarded(to_here, copy.start)

    def wait_send(name, par):
        for copy, to_here, _ in group(name, par):
            guarded(to_here, copy.wait_send)

    def wait_recv(name, par):
        for copy, _, from_here in group(name, par):
            guarded(from_here, copy.wait_recv)

    chunks = [("x", n) for n in range(lanes_of)]
    every = chunks + [("y", "face"), ("z", "face"), ("y", "inner"), ("z", "inner")]

    lane = lax.broadcasted_iota(jnp.int32, (8, LANES), 1)
    group_of, place = lane // 8, lane % 8

    def packed(value, g, total):
        return jnp.where(group_of == g, pltpu.roll(value, (W + 8 * g) % LANES, 1), total)

    def rows(j):
        return pl.ds(T + j, 8, stride=lanes_of)

    zero = jnp.zeros((8, LANES), jnp.float32)
    ends = ((0, 0, 0), (1, 1, nx - slabs))

    loads[0].wait()
    for side, slot, first in ends:
        total = zero
        for a in range(slabs):
            for j in range(lanes_of):
                value = field[0, first + a, rows(j), :]
                face[0, side, j, a] = value
                total = packed(value, a * lanes_of + j, total)
        pack[0, slot] = total
    peers = 2
    for sides in targets[1:]:
        for _, present in sides:
            peers = peers + present.astype(jnp.int32)
    pl.semaphore_wait(barrier, peers)
    for name in chunks + [("y", "face"), ("z", "face"), ("y", "inner")]:
        start(name, 0)

    def first_pack(m, carry):
        total = zero
        for a in range(slabs):
            for j in range(lanes_of):
                total = packed(field[0, m * slabs + slabs + a, rows(j), :], a * lanes_of + j, total)
        pack[0, 2 + m] = total
        return carry

    lax.fori_loop(0, inner, first_pack, 0)
    start(("z", "inner"), 0)

    loads[2].wait()
    squares = [vel_ref[n] * vel_ref[n] for n in range(vel_ref.shape[0])]

    def rate_slab(x, carry):
        codes = code[x]
        value = jnp.full(codes.shape, squares[0], jnp.float32)
        for n in range(1, len(squares)):
            value = jnp.where(codes == n, squares[n], value)
        rate[x] = value
        return carry

    lax.fori_loop(0, nx, rate_slab, 0)

    count = src_ref.shape[0]
    row_at = jnp.full((1, LANES), -1, jnp.int32)
    lane_row = lax.broadcasted_iota(jnp.int32, (1, LANES), 1)
    slot_col = lax.broadcasted_iota(jnp.int32, (LANES, LANES), 0)
    z_at = jnp.full((LANES, LANES), -1, jnp.int32)
    for s in range(count):
        cell = src_ref[s]
        sx = cell // (grid_y * grid_z) - ix * nx
        sy = cell // grid_z % grid_y - iy * ny
        sz = cell % grid_z - iz * nz
        here = (sx >= 0) & (sx < nx) & (sy >= 0) & (sy < ny)
        local = jnp.where(here, sx * ny + sy, -1)
        row_at = jnp.where((lane_row % count == s) & (lane_row < 3 * count), local, row_at)
        z_at = jnp.where((slot_col % count == s) & (slot_col < 3 * count), sz, z_at)
    spread = (z_at == lax.broadcasted_iota(jnp.int32, (LANES, LANES), 1)).astype(jnp.float32).astype(jnp.bfloat16)

    def source_field(t):
        wave = jnp.zeros((1, LANES), jnp.float32)
        for s in range(count):
            wave = jnp.where(lane_row % count == s, wave_ref[t, s], wave)
        high = wave.astype(jnp.bfloat16).astype(jnp.float32)
        rest = wave - high
        middle = rest.astype(jnp.bfloat16).astype(jnp.float32)
        parts = jnp.where(lane_row < count, high, jnp.where(lane_row < 2 * count, middle, rest - middle))
        block = slabs * ny

        def chunk(m, carry):
            row = lax.broadcasted_iota(jnp.int32, (block, LANES), 0) + m * block
            picks = jnp.where(row == row_at, parts, 0.0).astype(jnp.bfloat16)
            value = jnp.dot(picks, spread, preferred_element_type=jnp.float32)
            source[pl.ds(m * slabs, slabs)] = value.reshape(slabs, ny, LANES)
            return carry

        lax.fori_loop(0, packs, chunk, 0)

    near_edge = (lane < W) | (lane >= LANES - W)
    take_up = [jnp.where((place >= W) & (place - k < W), WEIGHTS[k - 1], 0.0) for k in range(1, W + 1)]
    take_down = [jnp.where((place < W) & (place + k >= W), WEIGHTS[k - 1], 0.0) for k in range(1, W + 1)]

    def edge_fix(cur, slot):
        delta = jnp.where(place < W, edge[cur, 0, slot], edge[cur, 1, slot]) - pack[cur, slot]
        fix = zero
        for k in range(1, W + 1):
            fix = fix + take_up[k - 1] * pltpu.roll(delta, k, 1)
            fix = fix + take_down[k - 1] * pltpu.roll(delta, LANES - k, 1)
        return fix

    def cell_row(cur, nxt, x, a, j, fix, layer):
        def shifted(k):
            return field[cur, x, pl.ds(T + j + k, 8, stride=lanes_of), :]

        f = shifted(0)
        acc = (3.0 * CENTRE) * f
        for k in range(1, W + 1):
            acc = acc + WEIGHTS[k - 1] * ((layer(k) + layer(-k)) + (shifted(k) + shifted(-k)))
        below, above = pltpu.roll(f, 1, 1), pltpu.roll(f, LANES - 1, 1)
        far_below = C4 * below + C3 * f + C2 * above
        far_above = C2 * below + C3 * f + C4 * above
        acc = acc + C1 * (below + above)
        acc = acc + pltpu.roll(far_below, 3, 1) + pltpu.roll(far_above, LANES - 3, 1)
        back = (2 * LANES - W - 8 * (a * lanes_of + j)) % LANES
        acc = acc + jnp.where(near_edge, pltpu.roll(fix, back, 1), 0.0)
        own = pl.ds(j, 8, stride=lanes_of)
        return (2.0 * f - field[nxt, x, rows(j), :]) + rate[x, own, :] * acc + source[x, own, :]

    loads[1].wait()
    for t in range(STEPS):
        cur, nxt = t % 2, (t + 1) % 2
        last = t == STEPS - 1

        def put(x, j, value):
            own = pl.ds(j, 8, stride=lanes_of)
            if last:
                out_ref[x, own, :] = value
            else:
                field[nxt, x, rows(j), :] = value
            if t == STEPS - 2:
                prev_ref[x, own, :] = value

        source_field(t)
        if t >= 1:
            for name in every:
                wait_send(name, nxt)
        wait_recv(("z", "face"), cur)
        wait_recv(("y", "face"), cur)
        fixes = [edge_fix(cur, slot) for _, slot, _ in ends]
        totals = [zero, zero]
        for j in range(lanes_of):
            wait_recv(("x", j), cur)
            for side, slot, first in ends:
                for a in range(slabs):
                    x = first + a

                    def layer(k, x=x, j=j):
                        if x + k < 0:
                            return halo[cur, 0, j, x + k + W]
                        if x + k >= nx:
                            return halo[cur, 1, j, x + k - nx]
                        return field[cur, x + k, rows(j), :]

                    value = cell_row(cur, nxt, x, a, j, fixes[slot], layer)
                    put(x, j, value)
                    if not last:
                        face[nxt, side, j, a] = value
                        totals[slot] = packed(value, a * lanes_of + j, totals[slot])
            if not last:
                start(("x", j), nxt)
        if not last:
            for _, slot, _ in ends:
                pack[nxt, slot] = totals[slot]
            start(("z", "face"), nxt)
            start(("y", "face"), nxt)
        wait_recv(("z", "inner"), cur)
        wait_recv(("y", "inner"), cur)

        def block(m, carry):
            fix = edge_fix(cur, 2 + m)
            total = zero
            for a in range(slabs):
                x = m * slabs + slabs + a
                for j in range(lanes_of):
                    value = cell_row(cur, nxt, x, a, j, fix, lambda k: field[cur, x + k, rows(j), :])
                    put(x, j, value)
                    if not last:
                        total = packed(value, a * lanes_of + j, total)
            if not last:
                pack[nxt, 2 + m] = total
            return carry

        lax.fori_loop(0, inner, block, 0)
        if not last:
            start(("z", "inner"), nxt)
            start(("y", "inner"), nxt)
    for name in every:
        wait_send(name, (STEPS - 1) % 2)


def solution(mesh):
    counts = tuple(mesh.shape[name] for name in ("gx", "gy", "gz"))

    def per_device(now, before, codes, velocity, wavelet, source_cell):
        nx, ny, nz = now.shape
        anywhere = pl.BlockSpec(memory_space=pl.ANY)
        scalars = pl.BlockSpec(memory_space=pltpu.SMEM)
        packs = nx * ny // LANES
        copies = 2 * (ny // 8) + 10
        return pl.pallas_call(
            functools.partial(kernel, (now.shape, counts)),
            out_shape=(pltpu.VMEM(now.shape, jnp.float32),) * 2,
            in_specs=[anywhere] * 3 + [scalars] * 3,
            out_specs=(pl.BlockSpec(memory_space=pltpu.VMEM),) * 2,
            scratch_shapes=[
                pltpu.VMEM((2, nx, ny + 2 * T, nz), jnp.float32),
                pltpu.VMEM((2, 2, ny // 8, W, 8, nz), jnp.float32),
                pltpu.VMEM((2, 2, ny // 8, W, 8, nz), jnp.float32),
                pltpu.VMEM((nx, ny, nz), jnp.float32),
                pltpu.VMEM((nx, ny, nz), jnp.int32),
                pltpu.VMEM((nx, ny, nz), jnp.float32),
                pltpu.VMEM((2, packs, 8, LANES), jnp.float32),
                pltpu.VMEM((2, 2, packs, 8, LANES), jnp.float32),
                pltpu.SemaphoreType.DMA((2, copies)),
                pltpu.SemaphoreType.DMA((2, copies)),
                pltpu.SemaphoreType.DMA((3,)),
            ],
            compiler_params=pltpu.CompilerParams(collective_id=0, has_side_effects=True),
        )(now, before, codes, velocity, wavelet, source_cell)

    block = P("gx", "gy", "gz")
    return jax.shard_map(
        per_device,
        mesh=mesh,
        in_specs=(block, block, block, P(), P(), P()),
        out_specs=(block, block),
        check_vma=False,
    )
```

```python
import functools

import jax
import jax.numpy as jnp
from jax import lax
from jax.experimental import pallas as pl
from jax.experimental.pallas import tpu as pltpu
from jax.sharding import PartitionSpec as P

STEPS = 6
CENTRE = -205.0 / 72.0
C1, C2, C3, C4 = (8.0 / 5.0, -1.0 / 5.0, 8.0 / 315.0, -1.0 / 560.0)
WEIGHTS = (C1, C2, C3, C4)
W = 4
CHUNKS = 2
T = 8
LANES = 128
MESH = pl.DeviceIdType.MESH
def kernel(sizes, now_hbm, before_hbm, code_hbm, vel_ref, wave_ref, src_ref, out_ref, prev_ref,
           field, state, halo, rate, code, source, pack, edge, send_sem, recv_sem, load_sem):
    (nx, ny, nz), (gx, gy, gz) = sizes
    grid_y, grid_z = ny * gy, nz * gz
    lanes_of = ny // 8
    slabs = LANES // 8 // lanes_of
    packs = nx // slabs
    ix, iy, iz = lax.axis_index("gx"), lax.axis_index("gy"), lax.axis_index("gz")
    targets = (
        (({"gx": lax.rem(ix + gx - 1, gx)}, None), ({"gx": lax.rem(ix + 1, gx)}, None)),
        (({"gy": iy - 1}, iy > 0), ({"gy": iy + 1}, iy < gy - 1)),
        (({"gz": iz - 1}, iz > 0), ({"gz": iz + 1}, iz < gz - 1)),
    )

    def guarded(condition, action):
        if condition is None:
            action()
        else:
            pl.when(condition)(action)

    own_x, own_y = pl.ds(0, nx), pl.ds(T, ny)
    half = lanes_of // CHUNKS
    loads = [
        pltpu.make_async_copy(now_hbm, field.at[0, own_x, own_y], load_sem.at[0]),
        pltpu.make_async_copy(before_hbm, field.at[1, own_x, own_y], load_sem.at[1]),
        pltpu.make_async_copy(code_hbm, code, load_sem.at[2]),
    ]
    for load in loads:
        load.start()

    nothing = jnp.zeros((nx, T, LANES), jnp.float32)
    for par in range(2):
        field[par, own_x, 0:T, :] = nothing
        field[par, own_x, pl.ds(T + ny, T), :] = nothing
    edge[...] = jnp.zeros_like(edge)

    barrier = pltpu.get_barrier_semaphore()
    for sides in targets:
        for target, present in sides:
            guarded(present, lambda target=target: pl.semaphore_signal(
                barrier, inc=1, device_id=target, device_id_type=MESH))

    inner = packs - 2

    def group(name, par):
        pieces = []
        if name[0] == "x":
            base = 2 * name[1]
            part = pl.ds(name[1] * half, half)
            pieces = [(0, state.at[par, pl.ds(0, W), part], halo.at[par, 1, name[1]]),
                      (0, state.at[par, pl.ds(nx - W, W), part], halo.at[par, 0, name[1]])]
        else:
            axis = 1 if name[0] == "y" else 2
            base = 2 * CHUNKS + (0 if axis == 1 else 6)
            if axis == 1:
                low, high = pl.ds(T, T), pl.ds(ny, T)
                over, under = pl.ds(T + ny, T), pl.ds(0, T)
                if name[1] == "face":
                    spans = [pl.ds(0, slabs), pl.ds(nx - slabs, slabs)]
                else:
                    spans = [pl.ds(slabs, nx - 2 * slabs)]
                    base = base + 4
                for span in spans:
                    pieces.append((1, field.at[par, span, low], field.at[par, span, over]))
                    pieces.append((1, field.at[par, span, high], field.at[par, span, under]))
            else:
                span = pl.ds(0, 2) if name[1] == "face" else pl.ds(2, inner)
                base = base + (0 if name[1] == "face" else 2)
                pieces.append((2, pack.at[par, span], edge.at[par, 1, span]))
                pieces.append((2, pack.at[par, span], edge.at[par, 0, span]))
        result = []
        for n, (axis, src, dst) in enumerate(pieces):
            target, present = targets[axis][n % 2]
            copy = pltpu.make_async_remote_copy(
                src_ref=src, dst_ref=dst, send_sem=send_sem.at[par, base + n], recv_sem=recv_sem.at[par, base + n],
                device_id=target, device_id_type=MESH)
            result.append((copy, present, targets[axis][1 - n % 2][1]))
        return result

    def start(name, par):
        for copy, to_here, _ in group(name, par):
            guarded(to_here, copy.start)

    def wait_send(name, par):
        for copy, to_here, _ in group(name, par):
            guarded(to_here, copy.wait_send)

    def wait_recv(name, par):
        for copy, _, from_here in group(name, par):
            guarded(from_here, copy.wait_recv)

    chunks = [("x", n) for n in range(CHUNKS)]
    every = chunks + [("y", "face"), ("z", "face"), ("y", "inner"), ("z", "inner")]

    lane = lax.broadcasted_iota(jnp.int32, (8, LANES), 1)
    group_of, place = lane // 8, lane % 8

    def packed(value, g, total):
        return jnp.where(group_of == g, pltpu.roll(value, (W + 8 * g) % LANES, 1), total)

    def rows(j):
        return pl.ds(T + j, 8, stride=lanes_of)

    zero = jnp.zeros((8, LANES), jnp.float32)
    ends = ((0, 0, 0), (1, 1, nx - slabs))

    loads[0].wait()
    for side, slot, first in ends:
        total = zero
        for a in range(slabs):
            for j in range(lanes_of):
                value = field[0, first + a, rows(j), :]
                state[0, first + a, j] = value
                total = packed(value, a * lanes_of + j, total)
        pack[0, slot] = total
    peers = 2
    for sides in targets[1:]:
        for _, present in sides:
            peers = peers + present.astype(jnp.int32)
    pl.semaphore_wait(barrier, peers)
    for name in chunks + [("y", "face"), ("z", "face"), ("y", "inner")]:
        start(name, 0)

    def first_pack(m, carry):
        total = zero
        for a in range(slabs):
            for j in range(lanes_of):
                value = field[0, m * slabs + slabs + a, rows(j), :]
                state[0, m * slabs + slabs + a, j] = value
                total = packed(value, a * lanes_of + j, total)
        pack[0, 2 + m] = total
        return carry

    lax.fori_loop(0, inner, first_pack, 0)
    start(("z", "inner"), 0)

    loads[2].wait()
    squares = [vel_ref[n] * vel_ref[n] for n in range(vel_ref.shape[0])]

    def rate_slab(x, carry):
        for j in range(lanes_of):
            codes = code[x, pl.ds(j, 8, stride=lanes_of), :]
            value = jnp.full(codes.shape, squares[0], jnp.float32)
            for n in range(1, len(squares)):
                value = jnp.where(codes == n, squares[n], value)
            rate[x, j] = value
        return carry

    lax.fori_loop(0, nx, rate_slab, 0)

    count = src_ref.shape[0]
    row_at = jnp.full((1, LANES), -1, jnp.int32)
    lane_row = lax.broadcasted_iota(jnp.int32, (1, LANES), 1)
    slot_col = lax.broadcasted_iota(jnp.int32, (LANES, LANES), 0)
    z_at = jnp.full((LANES, LANES), -1, jnp.int32)
    for s in range(count):
        cell = src_ref[s]
        sx = cell // (grid_y * grid_z) - ix * nx
        sy = cell // grid_z % grid_y - iy * ny
        sz = cell % grid_z - iz * nz
        here = (sx >= 0) & (sx < nx) & (sy >= 0) & (sy < ny)
        local = jnp.where(here, sx * ny + sy % lanes_of * 8 + sy // lanes_of, -1)
        row_at = jnp.where((lane_row % count == s) & (lane_row < 3 * count), local, row_at)
        z_at = jnp.where((slot_col % count == s) & (slot_col < 3 * count), sz, z_at)
    spread = (z_at == lax.broadcasted_iota(jnp.int32, (LANES, LANES), 1)).astype(jnp.float32).astype(jnp.bfloat16)

    def source_field(t):
        wave = jnp.zeros((1, LANES), jnp.float32)
        for s in range(count):
            wave = jnp.where(lane_row % count == s, wave_ref[t, s], wave)
        high = wave.astype(jnp.bfloat16).astype(jnp.float32)
        rest = wave - high
        middle = rest.astype(jnp.bfloat16).astype(jnp.float32)
        parts = jnp.where(lane_row < count, high, jnp.where(lane_row < 2 * count, middle, rest - middle))
        block = slabs * ny

        def chunk(m, carry):
            row = lax.broadcasted_iota(jnp.int32, (block, LANES), 0) + m * block
            picks = jnp.where(row == row_at, parts, 0.0).astype(jnp.bfloat16)
            value = jnp.dot(picks, spread, preferred_element_type=jnp.float32)
            source[pl.ds(m * slabs, slabs)] = value.reshape(slabs, lanes_of, 8, LANES)
            return carry

        lax.fori_loop(0, packs, chunk, 0)

    near_edge = (lane < W) | (lane >= LANES - W)
    take_up = [jnp.where((place >= W) & (place - k < W), WEIGHTS[k - 1], 0.0) for k in range(1, W + 1)]
    take_down = [jnp.where((place < W) & (place + k >= W), WEIGHTS[k - 1], 0.0) for k in range(1, W + 1)]

    def edge_fix(cur, slot):
        delta = jnp.where(place < W, edge[cur, 0, slot], edge[cur, 1, slot]) - pack[cur, slot]
        fix = zero
        for k in range(1, W + 1):
            fix = fix + take_up[k - 1] * pltpu.roll(delta, k, 1)
            fix = fix + take_down[k - 1] * pltpu.roll(delta, LANES - k, 1)
        return fix

    def cell_rows(cur, nxt, x, a, js, fix, layer):
        shifted = {}
        for o in range(js[0] - W, js[-1] + W + 1):
            if 0 <= o < lanes_of:
                shifted[o] = state[cur, x, o]
            else:
                shifted[o] = field[cur, x, pl.ds(T + o, 8, stride=lanes_of), :]
        values = []
        for j in js:
            f = shifted[j]
            acc = (3.0 * CENTRE) * f
            for k in range(1, W + 1):
                acc = acc + WEIGHTS[k - 1] * ((layer(k, j) + layer(-k, j)) + (shifted[j + k] + shifted[j - k]))
            below, above = pltpu.roll(f, 1, 1), pltpu.roll(f, LANES - 1, 1)
            far_below = C4 * below + C3 * f + C2 * above
            far_above = C2 * below + C3 * f + C4 * above
            acc = acc + C1 * (below + above)
            acc = acc + pltpu.roll(far_below, 3, 1) + pltpu.roll(far_above, LANES - 3, 1)
            back = (2 * LANES - W - 8 * (a * lanes_of + j)) % LANES
            acc = acc + jnp.where(near_edge, pltpu.roll(fix, back, 1), 0.0)
            values.append((2.0 * f - state[nxt, x, j]) + rate[x, j] * acc + source[x, j])
        return values

    def first_before(x, carry):
        for j in range(lanes_of):
            state[1, x, j] = field[1, x, rows(j), :]
        return carry

    loads[1].wait()
    lax.fori_loop(0, nx, first_before, 0)
    for t in range(STEPS):
        cur, nxt = t % 2, (t + 1) % 2
        last = t == STEPS - 1

        def put(x, j, value):
            own = pl.ds(j, 8, stride=lanes_of)
            if last:
                out_ref[x, own, :] = value
            else:
                state[nxt, x, j] = value
                field[nxt, x, rows(j), :] = value
            if t == STEPS - 2:
                prev_ref[x, own, :] = value

        source_field(t)
        if t >= 1:
            for name in every:
                wait_send(name, nxt)
        wait_recv(("z", "face"), cur)
        wait_recv(("y", "face"), cur)
        fixes = [edge_fix(cur, slot) for _, slot, _ in ends]
        totals = [zero, zero]
        for n in range(CHUNKS):
            wait_recv(("x", n), cur)
            js = range(n * half, n * half + half)
            for side, slot, first in ends:
                for a in range(slabs):
                    x = first + a

                    def layer(k, j, x=x, n=n):
                        if x + k < 0:
                            return halo[cur, 0, n, x + k + W, j - n * half]
                        if x + k >= nx:
                            return halo[cur, 1, n, x + k - nx, j - n * half]
                        return state[cur, x + k, j]

                    for j, value in zip(js, cell_rows(cur, nxt, x, a, js, fixes[slot], layer)):
                        put(x, j, value)
                        if not last:
                            totals[slot] = packed(value, a * lanes_of + j, totals[slot])
            if not last:
                start(("x", n), nxt)
        if not last:
            for _, slot, _ in ends:
                pack[nxt, slot] = totals[slot]
            start(("z", "face"), nxt)
            start(("y", "face"), nxt)
        wait_recv(("z", "inner"), cur)
        wait_recv(("y", "inner"), cur)

        def block(m, carry):
            fix = edge_fix(cur, 2 + m)
            total = zero
            for a in range(slabs):
                x = m * slabs + slabs + a
                js = range(lanes_of)
                near = lambda k, j: state[cur, x + k, j]
                for j, value in zip(js, cell_rows(cur, nxt, x, a, js, fix, near)):
                    put(x, j, value)
                    if not last:
                        total = packed(value, a * lanes_of + j, total)
            if not last:
                pack[nxt, 2 + m] = total
            return carry

        lax.fori_loop(0, inner, block, 0)
        if not last:
            start(("z", "inner"), nxt)
            start(("y", "inner"), nxt)
    for name in every:
        wait_send(name, (STEPS - 1) % 2)


def move_out(first_ref, second_ref, first_out, second_out, sem):
    moves = [
        pltpu.make_async_copy(first_ref, first_out, sem.at[0]),
        pltpu.make_async_copy(second_ref, second_out, sem.at[1]),
    ]
    for move in moves:
        move.start()
    for move in moves:
        move.wait()


def solution(mesh):
    counts = tuple(mesh.shape[name] for name in ("gx", "gy", "gz"))

    def per_device(now, before, codes, velocity, wavelet, source_cell):
        nx, ny, nz = now.shape
        anywhere = pl.BlockSpec(memory_space=pl.ANY)
        scalars = pl.BlockSpec(memory_space=pltpu.SMEM)
        packs = nx * ny // LANES
        copies = 2 * CHUNKS + 10
        results = pl.pallas_call(
            functools.partial(kernel, (now.shape, counts)),
            out_shape=(pltpu.VMEM(now.shape, jnp.float32),) * 2,
            in_specs=[anywhere] * 3 + [scalars] * 3,
            out_specs=(pl.BlockSpec(memory_space=pltpu.VMEM),) * 2,
            scratch_shapes=[
                pltpu.VMEM((2, nx, ny + 2 * T, nz), jnp.float32),
                pltpu.VMEM((2, nx, ny // 8, 8, nz), jnp.float32),
                pltpu.VMEM((2, 2, CHUNKS, W, ny // 8 // CHUNKS, 8, nz), jnp.float32),
                pltpu.VMEM((nx, ny // 8, 8, nz), jnp.float32),
                pltpu.VMEM((nx, ny, nz), jnp.int32),
                pltpu.VMEM((nx, ny // 8, 8, nz), jnp.float32),
                pltpu.VMEM((2, packs, 8, LANES), jnp.float32),
                pltpu.VMEM((2, 2, packs, 8, LANES), jnp.float32),
                pltpu.SemaphoreType.DMA((2, copies)),
                pltpu.SemaphoreType.DMA((2, copies)),
                pltpu.SemaphoreType.DMA((3,)),
            ],
            compiler_params=pltpu.CompilerParams(collective_id=0, has_side_effects=True),
        )(now, before, codes, velocity, wavelet, source_cell)
        return pl.pallas_call(
            move_out,
            out_shape=(jax.ShapeDtypeStruct(now.shape, jnp.float32),) * 2,
            in_specs=[pl.BlockSpec(memory_space=pltpu.VMEM)] * 2,
            out_specs=(anywhere, anywhere),
            scratch_shapes=[pltpu.SemaphoreType.DMA((2,))],
            compiler_params=pltpu.CompilerParams(vmem_limit_bytes=2**20),
        )(*[pltpu.with_memory_space_constraint(value, pltpu.VMEM) for value in results])

    block = P("gx", "gy", "gz")
    return jax.shard_map(
        per_device,
        mesh=mesh,
        in_specs=(block, block, block, P(), P(), P()),
        out_specs=(block, block),
        check_vma=False,
    )
```

```python
import functools

import jax
import jax.numpy as jnp
from jax import lax
from jax.experimental import pallas as pl
from jax.experimental.pallas import tpu as pltpu
from jax.sharding import PartitionSpec as P

STEPS = 6
CENTRE = -205.0 / 72.0
C1, C2, C3, C4 = (8.0 / 5.0, -1.0 / 5.0, 8.0 / 315.0, -1.0 / 560.0)
WEIGHTS = (C1, C2, C3, C4)
W = 4
CHUNKS = 1
T = 8
LANES = 128
MESH = pl.DeviceIdType.MESH
def kernel(sizes, now_hbm, before_hbm, code_hbm, vel_ref, wave_ref, src_ref, out_ref, prev_ref,
           field0, field1, state0, state1, pack0, pack1, halo, rate, code, source, edge, send_sem, recv_sem, load_sem):
    field, state, pack = (field0, field1), (state0, state1), (pack0, pack1)
    (nx, ny, nz), (gx, gy, gz) = sizes
    grid_y, grid_z = ny * gy, nz * gz
    lanes_of = ny // 8
    slabs = LANES // 8 // lanes_of
    packs = nx // slabs
    ix, iy, iz = lax.axis_index("gx"), lax.axis_index("gy"), lax.axis_index("gz")
    targets = (
        (({"gx": lax.rem(ix + gx - 1, gx)}, None), ({"gx": lax.rem(ix + 1, gx)}, None)),
        (({"gy": iy - 1}, iy > 0), ({"gy": iy + 1}, iy < gy - 1)),
        (({"gz": iz - 1}, iz > 0), ({"gz": iz + 1}, iz < gz - 1)),
    )

    def guarded(condition, action):
        if condition is None:
            action()
        else:
            pl.when(condition)(action)

    own_x, own_y = pl.ds(0, nx), pl.ds(T, ny)
    half = lanes_of // CHUNKS
    loads = [
        pltpu.make_async_copy(now_hbm, field[0].at[own_x, own_y], load_sem.at[0]),
        pltpu.make_async_copy(before_hbm, field[1].at[own_x, own_y], load_sem.at[1]),
        pltpu.make_async_copy(code_hbm, code, load_sem.at[2]),
    ]
    for load in loads:
        load.start()

    nothing = jnp.zeros((nx, T, LANES), jnp.float32)
    for par in range(2):
        field[par][own_x, 0:T, :] = nothing
        field[par][own_x, pl.ds(T + ny, T), :] = nothing
    edge[...] = jnp.zeros_like(edge)

    barrier = pltpu.get_barrier_semaphore()
    for sides in targets:
        for target, present in sides:
            guarded(present, lambda target=target: pl.semaphore_signal(
                barrier, inc=1, device_id=target, device_id_type=MESH))

    inner = packs - 2

    def group(name, par):
        pieces = []
        if name[0] == "x":
            base = 2 * name[1]
            part = pl.ds(name[1] * half, half)
            pieces = [(0, state[par].at[pl.ds(0, W), part], halo.at[par, 1, name[1]]),
                      (0, state[par].at[pl.ds(nx - W, W), part], halo.at[par, 0, name[1]])]
        else:
            axis = 1 if name[0] == "y" else 2
            base = 2 * CHUNKS + (0 if axis == 1 else 6)
            if axis == 1:
                low, high = pl.ds(T, T), pl.ds(ny, T)
                over, under = pl.ds(T + ny, T), pl.ds(0, T)
                if name[1] == "face":
                    spans = [pl.ds(0, slabs), pl.ds(nx - slabs, slabs)]
                else:
                    spans = [pl.ds(slabs, nx - 2 * slabs)]
                    base = base + 4
                for span in spans:
                    pieces.append((1, field[par].at[span, low], field[par].at[span, over]))
                    pieces.append((1, field[par].at[span, high], field[par].at[span, under]))
            else:
                span = pl.ds(0, 2) if name[1] == "face" else pl.ds(2, inner)
                base = base + (0 if name[1] == "face" else 2)
                pieces.append((2, pack[par].at[span], edge.at[par, 1, span]))
                pieces.append((2, pack[par].at[span], edge.at[par, 0, span]))
        result = []
        for n, (axis, src, dst) in enumerate(pieces):
            target, present = targets[axis][n % 2]
            copy = pltpu.make_async_remote_copy(
                src_ref=src, dst_ref=dst, send_sem=send_sem.at[par, base + n], recv_sem=recv_sem.at[par, base + n],
                device_id=target, device_id_type=MESH)
            result.append((copy, present, targets[axis][1 - n % 2][1]))
        return result

    def start(name, par):
        for copy, to_here, _ in group(name, par):
            guarded(to_here, copy.start)

    def wait_send(name, par):
        for copy, to_here, _ in group(name, par):
            guarded(to_here, copy.wait_send)

    def wait_recv(name, par):
        for copy, _, from_here in group(name, par):
            guarded(from_here, copy.wait_recv)

    chunks = [("x", n) for n in range(CHUNKS)]
    every = chunks + [("y", "face"), ("z", "face"), ("y", "inner"), ("z", "inner")]

    lane = lax.broadcasted_iota(jnp.int32, (8, LANES), 1)
    group_of, place = lane // 8, lane % 8

    def packed(value, g, total):
        return jnp.where(group_of == g, pltpu.roll(value, (W + 8 * g) % LANES, 1), total)

    def rows(j):
        return pl.ds(T + j, 8, stride=lanes_of)

    zero = jnp.zeros((8, LANES), jnp.float32)
    ends = ((0, 0, 0), (1, 1, nx - slabs))

    loads[0].wait()
    for side, slot, first in ends:
        total = zero
        for a in range(slabs):
            for j in range(lanes_of):
                value = field[0][first + a, rows(j), :]
                state[0][first + a, j] = value
                total = packed(value, a * lanes_of + j, total)
        pack[0][slot] = total
    peers = 2
    for sides in targets[1:]:
        for _, present in sides:
            peers = peers + present.astype(jnp.int32)
    pl.semaphore_wait(barrier, peers)
    for name in chunks + [("y", "face"), ("z", "face"), ("y", "inner")]:
        start(name, 0)

    def first_pack(m, carry):
        total = zero
        for a in range(slabs):
            for j in range(lanes_of):
                value = field[0][m * slabs + slabs + a, rows(j), :]
                state[0][m * slabs + slabs + a, j] = value
                total = packed(value, a * lanes_of + j, total)
        pack[0][2 + m] = total
        return carry

    lax.fori_loop(0, inner, first_pack, 0)
    start(("z", "inner"), 0)

    loads[2].wait()
    squares = [vel_ref[n] * vel_ref[n] for n in range(vel_ref.shape[0])]

    def rate_slab(x, carry):
        for j in range(lanes_of):
            codes = code[x, pl.ds(j, 8, stride=lanes_of), :]
            value = jnp.full(codes.shape, squares[0], jnp.float32)
            for n in range(1, len(squares)):
                value = jnp.where(codes == n, squares[n], value)
            rate[x, j] = value
        return carry

    lax.fori_loop(0, nx, rate_slab, 0)

    count = src_ref.shape[0]
    row_at = jnp.full((1, LANES), -1, jnp.int32)
    lane_row = lax.broadcasted_iota(jnp.int32, (1, LANES), 1)
    slot_col = lax.broadcasted_iota(jnp.int32, (LANES, LANES), 0)
    z_at = jnp.full((LANES, LANES), -1, jnp.int32)
    for s in range(count):
        cell = src_ref[s]
        sx = cell // (grid_y * grid_z) - ix * nx
        sy = cell // grid_z % grid_y - iy * ny
        sz = cell % grid_z - iz * nz
        here = (sx >= 0) & (sx < nx) & (sy >= 0) & (sy < ny)
        local = jnp.where(here, sx * ny + sy % lanes_of * 8 + sy // lanes_of, -1)
        row_at = jnp.where((lane_row % count == s) & (lane_row < 3 * count), local, row_at)
        z_at = jnp.where((slot_col % count == s) & (slot_col < 3 * count), sz, z_at)
    spread = (z_at == lax.broadcasted_iota(jnp.int32, (LANES, LANES), 1)).astype(jnp.float32).astype(jnp.bfloat16)

    def source_field(t):
        wave = jnp.zeros((1, LANES), jnp.float32)
        for s in range(count):
            wave = jnp.where(lane_row % count == s, wave_ref[t, s], wave)
        high = wave.astype(jnp.bfloat16).astype(jnp.float32)
        rest = wave - high
        middle = rest.astype(jnp.bfloat16).astype(jnp.float32)
        parts = jnp.where(lane_row < count, high, jnp.where(lane_row < 2 * count, middle, rest - middle))
        block = slabs * ny

        def chunk(m, carry):
            row = lax.broadcasted_iota(jnp.int32, (block, LANES), 0) + m * block
            picks = jnp.where(row == row_at, parts, 0.0).astype(jnp.bfloat16)
            value = jnp.dot(picks, spread, preferred_element_type=jnp.float32)
            source[pl.ds(m * slabs, slabs)] = value.reshape(slabs, lanes_of, 8, LANES)
            return carry

        lax.fori_loop(0, packs, chunk, 0)

    near_edge = (lane < W) | (lane >= LANES - W)
    take_up = [jnp.where((place >= W) & (place - k < W), WEIGHTS[k - 1], 0.0) for k in range(1, W + 1)]
    take_down = [jnp.where((place < W) & (place + k >= W), WEIGHTS[k - 1], 0.0) for k in range(1, W + 1)]

    def edge_fix(cur, slot):
        delta = jnp.where(place < W, edge[cur, 0, slot], edge[cur, 1, slot]) - pack[cur][slot]
        fix = zero
        for k in range(1, W + 1):
            fix = fix + take_up[k - 1] * pltpu.roll(delta, k, 1)
            fix = fix + take_down[k - 1] * pltpu.roll(delta, LANES - k, 1)
        return fix

    def cell_rows(cur, nxt, x, a, js, fix, layer):
        shifted = {}
        for o in range(js[0] - W, js[-1] + W + 1):
            if 0 <= o < lanes_of:
                shifted[o] = state[cur][x, o]
            else:
                shifted[o] = field[cur][x, pl.ds(T + o, 8, stride=lanes_of), :]
        values = []
        for j in js:
            f = shifted[j]
            acc = (3.0 * CENTRE) * f
            for k in range(1, W + 1):
                acc = acc + WEIGHTS[k - 1] * ((layer(k, j) + layer(-k, j)) + (shifted[j + k] + shifted[j - k]))
            below, above = pltpu.roll(f, 1, 1), pltpu.roll(f, LANES - 1, 1)
            far_below = C4 * below + C3 * f + C2 * above
            far_above = C2 * below + C3 * f + C4 * above
            acc = acc + C1 * (below + above)
            acc = acc + pltpu.roll(far_below, 3, 1) + pltpu.roll(far_above, LANES - 3, 1)
            back = (2 * LANES - W - 8 * (a * lanes_of + j)) % LANES
            acc = acc + jnp.where(near_edge, pltpu.roll(fix, back, 1), 0.0)
            values.append((2.0 * f - state[nxt][x, j]) + rate[x, j] * acc + source[x, j])
        return values

    def first_before(x, carry):
        for j in range(lanes_of):
            state[1][x, j] = field[1][x, rows(j), :]
        return carry

    loads[1].wait()
    lax.fori_loop(0, nx, first_before, 0)
    for t in range(STEPS):
        cur, nxt = t % 2, (t + 1) % 2
        last = t == STEPS - 1

        def put(x, j, value):
            own = pl.ds(j, 8, stride=lanes_of)
            if last:
                out_ref[x, own, :] = value
            else:
                state[nxt][x, j] = value
                field[nxt][x, rows(j), :] = value
            if t == STEPS - 2:
                prev_ref[x, own, :] = value

        source_field(t)
        if t >= 1:
            for name in every:
                wait_send(name, nxt)
        wait_recv(("z", "face"), cur)
        wait_recv(("y", "face"), cur)
        fixes = [edge_fix(cur, slot) for _, slot, _ in ends]
        totals = [zero, zero]
        for n in range(CHUNKS):
            wait_recv(("x", n), cur)
            js = range(n * half, n * half + half)
            for side, slot, first in ends:
                for a in range(slabs):
                    x = first + a

                    def layer(k, j, x=x, n=n):
                        if x + k < 0:
                            return halo[cur, 0, n, x + k + W, j - n * half]
                        if x + k >= nx:
                            return halo[cur, 1, n, x + k - nx, j - n * half]
                        return state[cur][x + k, j]

                    for j, value in zip(js, cell_rows(cur, nxt, x, a, js, fixes[slot], layer)):
                        put(x, j, value)
                        if not last:
                            totals[slot] = packed(value, a * lanes_of + j, totals[slot])
            if not last:
                start(("x", n), nxt)
        if not last:
            for _, slot, _ in ends:
                pack[nxt][slot] = totals[slot]
            start(("z", "face"), nxt)
            start(("y", "face"), nxt)
        wait_recv(("z", "inner"), cur)
        wait_recv(("y", "inner"), cur)

        def block(m, carry):
            fix = edge_fix(cur, 2 + m)
            total = zero
            for a in range(slabs):
                x = m * slabs + slabs + a
                js = range(lanes_of)
                near = lambda k, j: state[cur][x + k, j]
                for j, value in zip(js, cell_rows(cur, nxt, x, a, js, fix, near)):
                    put(x, j, value)
                    if not last:
                        total = packed(value, a * lanes_of + j, total)
            if not last:
                pack[nxt][2 + m] = total
            return carry

        lax.fori_loop(0, inner, block, 0)
        if not last:
            start(("z", "inner"), nxt)
            start(("y", "inner"), nxt)
    for name in every:
        wait_send(name, (STEPS - 1) % 2)


def move_out(first_ref, second_ref, first_out, second_out, sem):
    moves = [
        pltpu.make_async_copy(first_ref, first_out, sem.at[0]),
        pltpu.make_async_copy(second_ref, second_out, sem.at[1]),
    ]
    for move in moves:
        move.start()
    for move in moves:
        move.wait()


def solution(mesh):
    counts = tuple(mesh.shape[name] for name in ("gx", "gy", "gz"))

    def per_device(now, before, codes, velocity, wavelet, source_cell):
        nx, ny, nz = now.shape
        anywhere = pl.BlockSpec(memory_space=pl.ANY)
        scalars = pl.BlockSpec(memory_space=pltpu.SMEM)
        packs = nx * ny // LANES
        copies = 2 * CHUNKS + 10
        results = pl.pallas_call(
            functools.partial(kernel, (now.shape, counts)),
            out_shape=(pltpu.VMEM(now.shape, jnp.float32),) * 2,
            in_specs=[anywhere] * 3 + [scalars] * 3,
            out_specs=(pl.BlockSpec(memory_space=pltpu.VMEM),) * 2,
            scratch_shapes=[
                pltpu.VMEM((nx, ny + 2 * T, nz), jnp.float32),
                pltpu.VMEM((nx, ny + 2 * T, nz), jnp.float32),
                pltpu.VMEM((nx, ny // 8, 8, nz), jnp.float32),
                pltpu.VMEM((nx, ny // 8, 8, nz), jnp.float32),
                pltpu.VMEM((packs, 8, LANES), jnp.float32),
                pltpu.VMEM((packs, 8, LANES), jnp.float32),
                pltpu.VMEM((2, 2, CHUNKS, W, ny // 8 // CHUNKS, 8, nz), jnp.float32),
                pltpu.VMEM((nx, ny // 8, 8, nz), jnp.float32),
                pltpu.VMEM((nx, ny, nz), jnp.int32),
                pltpu.VMEM((nx, ny // 8, 8, nz), jnp.float32),
                pltpu.VMEM((2, 2, packs, 8, LANES), jnp.float32),
                pltpu.SemaphoreType.DMA((2, copies)),
                pltpu.SemaphoreType.DMA((2, copies)),
                pltpu.SemaphoreType.DMA((3,)),
            ],
            compiler_params=pltpu.CompilerParams(collective_id=0, has_side_effects=True),
        )(now, before, codes, velocity, wavelet, source_cell)
        return pl.pallas_call(
            move_out,
            out_shape=(jax.ShapeDtypeStruct(now.shape, jnp.float32),) * 2,
            in_specs=[pl.BlockSpec(memory_space=pltpu.VMEM)] * 2,
            out_specs=(anywhere, anywhere),
            scratch_shapes=[pltpu.SemaphoreType.DMA((2,))],
            compiler_params=pltpu.CompilerParams(vmem_limit_bytes=2**20),
        )(*[pltpu.with_memory_space_constraint(value, pltpu.VMEM) for value in results])

    block = P("gx", "gy", "gz")
    return jax.shard_map(
        per_device,
        mesh=mesh,
        in_specs=(block, block, block, P(), P(), P()),
        out_specs=(block, block),
        check_vma=False,
    )
```
